32 devices in a mesh: dp: 1 (over z), tp: 32 (over y, x, core).
Axes of the slice: x: 4, y: 4, z: 1, core: 2. Of those that a mesh axis runs over, the one named last changes fastest.
The devices are a block of a 4x4x8 slice.
Arguments:
- ids: int32 [16, 256], P('dp')
- E: bfloat16 [8192, 8192], P(None, 'tp')
- g: bfloat16 [8192], replicated
- W: bfloat16 [8192, 10240], P(None, 'tp')
- du: bfloat16 [16, 256, 10240], P('dp', None, 'tp')
- dres: bfloat16 [16, 256, 8192], P('dp', 'tp')
Outputs:
- output 1: bfloat16 [16, 256, 10240], P('dp', None, 'tp')
- output 2: bfloat16 [16, 256, 8192], P('dp', 'tp')
- output 3: float32 [8192, 8192], P('dp', 'tp')
- output 4: float32 [8192, 10240], P('dp', 'tp')
- output 5: float32 [8192], P('dp')
All inputs are finite; a program needn't handle non-finite values.
Results may differ from the reference program's by a relative error of at most 0.00618117.
Values are sent between devices in bfloat16 or wider.
A program may use at most 768 MiB of HBM per device.

```python
import jax
import jax.numpy as jnp
from jax import lax
import math

K = 16
T = 256
V = 8192
D = 8192
FC = 10240
EPS = 1e-6


def setup_inputs(seed: int = 0, part: int = 0) -> dict:
    key = jax.random.key(seed)
    kE, kg, kW, kpart = jax.random.split(key, 4)
    kp = jax.random.fold_in(kpart, part)
    k1, k2, k3, k4, k5, k6 = jax.random.split(kp, 6)
    scale = 1.0 / math.sqrt(K * T)
    dscale = scale * math.sqrt(D / FC)
    wscale = 1.0 / math.sqrt(D)
    E = jax.random.normal(kE, (V, D), jnp.float32).astype(jnp.bfloat16)
    g = (1.0 + 0.4 * jax.random.normal(kg, (D,), jnp.float32)).astype(jnp.bfloat16)
    W = (jax.random.normal(kW, (D, FC), jnp.float32) * wscale).astype(jnp.bfloat16)
    rand_bits = jax.random.bits(jax.random.fold_in(k1, 7), (K, T), jnp.uint32) >> 16
    square_part = (rand_bits * rand_bits) >> 16
    fourth_power = (square_part * square_part) >> 16
    ids = jnp.minimum(((fourth_power * (V >> 6)) >> 10).astype(jnp.int32), V - 1)
    du = (jax.random.normal(k5, (K, T, FC), jnp.float32) * dscale).astype(jnp.bfloat16)
    dres = (jax.random.normal(k6, (K, T, D), jnp.float32) * scale).astype(jnp.bfloat16)
    return dict(ids=ids, E=E, g=g, W=W, du=du, dres=dres)


def reference(ids, E, g, W, du, dres):
    gf = g.astype(jnp.float32)

    def step(carry, inp):
        dE, dW, dg = carry
        idk, duk, dresk = inp
        x = jnp.take(E, idk, axis=0)
        xf = x.astype(jnp.float32)
        rs = lax.rsqrt(jnp.mean(xf * xf, axis=-1, keepdims=True) + EPS)
        nh = xf * rs
        n = (nh * gf).astype(jnp.bfloat16)
        u = jnp.dot(n, W, preferred_element_type=jnp.float32).astype(jnp.bfloat16)
        dn = jnp.dot(duk, W.T, preferred_element_type=jnp.float32)
        gdn = gf * dn
        dx = dresk.astype(jnp.float32) + rs * (gdn - nh * jnp.mean(nh * gdn, axis=-1, keepdims=True))
        dE = dE.at[idk].add(dx)
        dW = dW + jnp.dot(n.T, duk, preferred_element_type=jnp.float32)
        dg = dg + jnp.sum(dn * nh, axis=0)
        return (dE, dW, dg), (u, x)

    init = (jnp.zeros((V, D), jnp.float32), jnp.zeros((D, FC), jnp.float32), jnp.zeros((D,), jnp.float32))
    (dE, dW, dg), (u, x) = lax.scan(step, init, (ids, du, dres))
    return u, x, dE, dW, dg
```

```python
import functools
import math

import jax
import jax.numpy as jnp
from jax import lax
from jax.experimental import pallas as pl
from jax.experimental.layout import Layout, with_layout_constraint
from jax.experimental.pallas import tpu as pltpu
from jax.sharding import PartitionSpec as P


EPS = 1e-6
f32 = jnp.float32
bf16 = jnp.bfloat16
LANES = 128
SPLIT = (11, 5)


def _gather_kernel(S, du_ref, wt_ref, dres_ref, ss_ref, du_r, du_c, w_r, w_c, dr_ref, sum_ref, vdu, vw, vdr, rbuf, mid, cbuf,
                   lsem, ssem, rsem, wssem, wrsem, dssem, drsem, tssem, trsem):
    me = lax.axis_index('tp')
    c = lax.rem(me, 2)
    x = lax.rem(me // 2, S)
    y = me // (2 * S)
    F, N = du_ref.shape
    H = N // 2
    dev = lambda yy, xx, cc: (yy * S + xx) * 2 + cc
    rot = lambda v, k: lax.rem(v + k, S)

    barrier = pltpu.get_barrier_semaphore()
    G = dres_ref.shape[1] // dr_ref.shape[2]
    for k in range(1, G):
        pl.semaphore_signal(barrier, inc=1, device_id={'tp': lax.rem(me + k, G)})
    pl.semaphore_wait(barrier, G - 1)

    i_row = lax.rem(me, 2 * S)
    row = []
    for k in range(1, 2 * S):
        cp = pltpu.make_async_remote_copy(
            ss_ref, rbuf.at[i_row], tssem.at[k], trsem.at[k], device_id={'tp': y * 2 * S + lax.rem(i_row + k, 2 * S)}
        )
        cp.start()
        row.append(cp)
    rbuf[i_row] = ss_ref[...]

    Bw = dr_ref.shape[2]
    wblock = lambda b: wt_ref.at[:, pl.ds(pl.multiple_of(b * Bw, Bw), Bw)]
    outs = []
    schemes = []
    for j, (pos, buf, wbuf) in enumerate(((x, du_r, w_r), (y, du_c, w_c))):
        at = (lambda k, cc: dev(y, rot(x, k), cc)) if j == 0 else (lambda k, cc: dev(rot(y, k), x, cc))
        src = du_ref.at[:, pl.ds(j * H, H)]
        schemes.append((j, pos, buf, wbuf, at, src, 2 * pos + c))

    def send(j, i, src, dst, p):
        cp = pltpu.make_async_remote_copy(src, dst, ssem.at[j, i], rsem.at[j, i], device_id={'tp': p})
        cp.start()
        outs.append(cp)
        return cp

    ring = []
    for j, pos, buf, wbuf, at, src, s in schemes:
        ring.append((send(j, 0, src, buf.at[s], at(1, c)), send(j, 1, src, buf.at[s], at(S - 1, c))))
    local = []
    for j, pos, buf, wbuf, at, src, s in schemes:
        own = [wblock(dev(t, x, c) if j == 0 else dev(y, t, c)) for t in range(S)]
        for i, (a, v) in enumerate([(src, vdu.at[j])] + [(own[t], vw.at[j, t]) for t in range(S)]):
            cp = pltpu.make_async_copy(a, v, lsem.at[j, i])
            cp.start()
            local.append((cp, v, buf.at[s] if i == 0 else wbuf.at[i - 1, s], j, i))
    cp = pltpu.make_async_copy(dres_ref.at[:, pl.ds(pl.multiple_of(me * dr_ref.shape[2], dr_ref.shape[2]), dr_ref.shape[2])], vdr, lsem.at[0, 10])
    cp.start()
    local.append((cp, vdr, dr_ref.at[me], 0, 10))
    for k in (1, S - 1, 0, 2):
        for j, pos, buf, wbuf, at, src, s in schemes:
            for cc in range(2):
                oc = c if cc == 0 else 1 - c
                if k == 0 and cc == 0:
                    continue
                for t in range(S):
                    blk = wblock(dev(t, rot(x, k), oc) if j == 0 else dev(rot(y, k), t, oc))
                    cp = pltpu.make_async_remote_copy(
                        blk, wbuf.at[t, s], wssem.at[j, 2 * k + cc, t], wrsem.at[j, 2 * k + cc, t], device_id={'tp': at(k, oc)}
                    )
                    cp.start()
                    outs.append(cp)
        if k == 1:
            for j, pos, buf, wbuf, at, src, s in schemes:
                send(j, 2, src, buf.at[s], at(0, 1 - c))
        if k == S - 1:
            for cp in row:
                cp.wait()
            total = rbuf[0]
            for t in range(1, 2 * S):
                total = total + rbuf[t]
            mid[...] = total
            cbuf[y] = total
            col = []
            for t in range(1, S):
                cp = pltpu.make_async_remote_copy(
                    mid, cbuf.at[y], tssem.at[2 * S + t], trsem.at[2 * S + t], device_id={'tp': dev(rot(y, t), x, c)}
                )
                cp.start()
                col.append(cp)
            halves = []
            for j, pos, buf, wbuf, at, src, s in schemes:
                right, left = ring[j]
                sl = 2 * rot(pos, S - 1) + c
                sr = 2 * rot(pos, 1) + c
                right.wait_recv()
                a = send(j, 3, buf.at[sl, pl.ds(0, F // 2)], buf.at[sl, pl.ds(0, F // 2)], at(1, c))
                left.wait_recv()
                b = send(j, 4, buf.at[sr, pl.ds(F // 2, F // 2)], buf.at[sr, pl.ds(F // 2, F // 2)], at(S - 1, c))
                send(j, 5, buf.at[sl], buf.at[sl], at(0, 1 - c))
                send(j, 6, buf.at[sr], buf.at[sr], at(0, 1 - c))
                halves.append((a, b))
    for k in range(1, G):
        p = lax.rem(me + k, G)
        cp = pltpu.make_async_remote_copy(
            dres_ref.at[:, pl.ds(pl.multiple_of(p * Bw, Bw), Bw)], dr_ref.at[me], dssem.at[k], drsem.at[k], device_id={'tp': p}
        )
        cp.start()
        outs.append(cp)
    for cp, v, dst, j, i in local:
        cp.wait()
    back = []
    for cp, v, dst, j, i in local:
        cb = pltpu.make_async_copy(v, dst, lsem.at[j, i + 5])
        cb.start()
        back.append(cb)
    for j, pos, buf, wbuf, at, src, s in schemes:
        a, b = halves[j]
        a.wait_recv()
        b.wait_recv()
        so = 2 * rot(pos, 2) + c
        send(j, 7, buf.at[so], buf.at[so], at(0, 1 - c))
    early = {id(cp) for pair in ring + halves for cp in pair}
    for cp in outs:
        cp.wait_send()
        if id(cp) not in early:
            cp.wait_recv()
    for cb in back:
        cb.wait()
    for cp in col:
        cp.wait()
    total = cbuf[0]
    for t in range(1, S):
        total = total + cbuf[t]
    sum_ref[...] = total


def _gather(duT, wt, dres, ss, S, cid):
    F, N = duT.shape
    G = 2 * S * S
    B = wt.shape[1] // G
    H = N // 2
    R = ss.shape[0]
    anyspace = pl.BlockSpec(memory_space=pl.ANY)
    vm = pl.BlockSpec(memory_space=pltpu.VMEM)
    dma = pltpu.SemaphoreType.DMA
    return pl.pallas_call(
        functools.partial(_gather_kernel, S),
        out_shape=(
            jax.ShapeDtypeStruct((2 * S, F, H), bf16),
            jax.ShapeDtypeStruct((2 * S, F, H), bf16),
            jax.ShapeDtypeStruct((S, 2 * S, F, B), bf16),
            jax.ShapeDtypeStruct((S, 2 * S, F, B), bf16),
            jax.ShapeDtypeStruct((G, dres.shape[0], B), bf16),
            jax.ShapeDtypeStruct((R, LANES), f32),
        ),
        in_specs=[anyspace, anyspace, anyspace, vm],
        out_specs=(anyspace,) * 5 + (vm,),
        scratch_shapes=[
            pltpu.VMEM((2, F, H), bf16),
            pltpu.VMEM((2, S, F, B), bf16),
            pltpu.VMEM((dres.shape[0], B), bf16),
            pltpu.VMEM((2 * S, R, LANES), f32),
            pltpu.VMEM((R, LANES), f32),
            pltpu.VMEM((S, R, LANES), f32),
            dma((2, 16)), dma((2, 8)), dma((2, 8)), dma((2, 2 * S, S)), dma((2, 2 * S, S)), dma((G,)), dma((G,)),
            dma((3 * S,)), dma((3 * S,)),
        ],
        compiler_params=pltpu.CompilerParams(collective_id=cid, has_side_effects=True),
        name='gather_du_w',
    )(duT, wt, dres, ss)


def _stats_kernel(C, ROW, S, Q, x_ref, sum_ref, gat_ref, rbuf, mid, cbuf, ssem, rsem, ssem2, rsem2):
    me = lax.axis_index('tp')
    y, i = me // ROW, lax.rem(me, ROW)
    barrier = pltpu.get_barrier_semaphore()
    row_peers = [y * ROW + lax.rem(i + k, ROW) for k in range(1, ROW)]
    col_peers = [lax.rem(y + k, C) * ROW + i for k in range(1, C)]
    for p in row_peers + col_peers:
        pl.semaphore_signal(barrier, inc=1, device_id={'tp': p})
    pl.semaphore_wait(barrier, ROW + C - 2)

    copies = []
    for k, p in enumerate(row_peers):
        cp = pltpu.make_async_remote_copy(x_ref, rbuf.at[i], ssem.at[k], rsem.at[k], device_id={'tp': p})
        cp.start()
        copies.append(cp)
    rbuf[i] = x_ref[...]
    for cp in copies:
        cp.wait()
    total = rbuf[0, :S]
    for s in range(1, ROW):
        total = total + rbuf[s, :S]
    mid[:S] = total
    if Q:
        for s in range(ROW):
            mid[S + s * Q:S + (s + 1) * Q] = rbuf[s, S:]

    copies = []
    for k, p in enumerate(col_peers):
        cp = pltpu.make_async_remote_copy(mid, cbuf.at[y], ssem2.at[k], rsem2.at[k], device_id={'tp': p})
        cp.start()
        copies.append(cp)
    cbuf[y] = mid[...]
    for cp in copies:
        cp.wait()
    total = cbuf[0, :S]
    for s in range(1, C):
        total = total + cbuf[s, :S]
    sum_ref[...] = total
    if Q:
        for s in range(C):
            gat_ref[s * ROW * Q:(s + 1) * ROW * Q] = cbuf[s, S:]
    else:
        gat_ref[...] = jnp.zeros_like(gat_ref)


def _stats(x, C, Q, cid):
    ROW = 2 * C
    R = x.shape[0]
    S = R - Q
    M = S + ROW * Q
    q_out = C * ROW * Q if Q else 8
    vm = pl.BlockSpec(memory_space=pltpu.VMEM)
    return pl.pallas_call(
        functools.partial(_stats_kernel, C, ROW, S, Q),
        out_shape=(jax.ShapeDtypeStruct((S, LANES), f32), jax.ShapeDtypeStruct((q_out, LANES), f32)),
        in_specs=[vm],
        out_specs=(vm, vm),
        scratch_shapes=[
            pltpu.VMEM((ROW, R, LANES), f32),
            pltpu.VMEM((M, LANES), f32),
            pltpu.VMEM((C, M, LANES), f32),
            pltpu.SemaphoreType.DMA((ROW - 1,)),
            pltpu.SemaphoreType.DMA((ROW - 1,)),
            pltpu.SemaphoreType.DMA((C - 1,)),
            pltpu.SemaphoreType.DMA((C - 1,)),
        ],
        compiler_params=pltpu.CompilerParams(collective_id=cid, has_side_effects=True),
    )(x)


def rowmajor(v):
    return with_layout_constraint(v, Layout(major_to_minor=tuple(range(v.ndim))))


def solution(mesh):
    G = mesh.shape['tp']
    S = math.isqrt(G // 2)
    C, ROW = S, 2 * S

    def shift(j, k):
        out = []
        for i in range(G):
            y, x, c = i // ROW, i // 2 % S, i % 2
            t = ((y + k) % S, x, c) if j == 0 else (y, (x + k) % S, c)
            out.append((i, (t[0] * S + t[1]) * 2 + t[2]))
        return out

    def body(ids, E, g, W, du, dres):
        K, T = ids.shape
        D = g.shape[0]
        B = E.shape[1]
        F = W.shape[1]
        N = K * T
        TL = T // G
        r = lax.axis_index('tp')
        idf = ids.reshape(N)
        gl = lax.dynamic_slice_in_dim(g, r * B, B).astype(f32)
        gf = g.astype(f32)
        duf = du.reshape(N, F)
        xl = rowmajor(jnp.take(E, idf, axis=0))
        xf = xl.astype(f32)
        ss = jnp.sum(xf * xf, axis=-1).reshape(N // LANES, LANES)
        duR, duC, wR, wC, dt, ss = _gather(duf.T, W.T, dres.reshape(K * TL, D),
                                           ss, S, 2)
        rs = lax.rsqrt(ss.reshape(N) / D + EPS)[:, None]
        dl = dt.reshape(G, K, TL, B).transpose(1, 0, 2, 3).reshape(N, B)
        duR, duC, wR, wC, rs, dl = lax.optimization_barrier((duR, duC, wR, wC, rs, dl))
        parts = []
        for j, (a, w, pos) in enumerate(((duR, wR, r // ROW), (duC, wC, lax.rem(r // 2, S)))):
            p = jnp.einsum('kt,ykb->ytb', a.reshape(ROW * F, N // 2), w.reshape(S, ROW * F, B),
                           preferred_element_type=f32).astype(bf16)
            p = rowmajor(p)
            ps = []
            for k in (1, 3, 2, 0):
                pk = lax.dynamic_index_in_dim(p, lax.rem(pos + k, S), 0, keepdims=False)
                ps.append(lax.ppermute(pk, 'tp', shift(j, k)) if k else pk)
            parts.append(ps)
        us, xss = [], []

        def forward(xg, at, kc, dW):
            sl = slice(at * T, (at + kc) * T)
            xss.append(lax.dynamic_slice_in_dim(xg.reshape(kc, T, D), r * TL, TL, axis=1))
            n = (xg.astype(f32) * rs[sl] * gf).astype(bf16)
            us.append(jnp.dot(n, W, preferred_element_type=f32).astype(bf16))
            w = jnp.einsum('td,tf->df', n, duf[sl], preferred_element_type=f32)
            return w if dW is None else dW + w

        k0, k1 = SPLIT
        x0 = lax.all_gather(xl[:k0 * T], 'tp', axis=1, tiled=True)
        x1 = lax.all_gather(xl[k0 * T:], 'tp', axis=1, tiled=True)
        dW = forward(x0, 0, k0, None)
        dW, us[0], parts = lax.optimization_barrier((dW, us[0], parts))
        dn = jnp.concatenate([sum(p.astype(f32) for p in ps) for ps in parts], axis=0)
        nh = xl.astype(f32) * rs
        gdn = gl * dn
        pk = jnp.concatenate([jnp.sum(nh * gdn, axis=-1).reshape(N // LANES, LANES),
                              jnp.sum(dn * nh, axis=0).reshape(B // LANES, LANES)], axis=0)
        ms, dgs = _stats(pk, C, B // LANES, 1)
        dg = dgs.reshape(D)
        dx = dl.astype(f32) + rs * (gdn - nh * (ms.reshape(N) / D)[:, None])
        dE = jnp.zeros(E.shape, f32).at[idf].add(dx)
        x1, dW, dE = lax.optimization_barrier((x1, dW, dE))
        dW = forward(x1, k0, k1, dW)
        u = jnp.concatenate(us, axis=0).reshape(K, T, F)
        xs = jnp.concatenate(xss, axis=0)
        return u, xs, dE, dW, dg

    return jax.shard_map(
        body,
        mesh=mesh,
        in_specs=(P('dp', None), P(None, 'tp'), P(), P(None, 'tp'), P('dp', None, 'tp'), P('dp', 'tp', None)),
        out_specs=(P('dp', None, 'tp'), P('dp', 'tp', None), P('dp', 'tp'), P('dp', 'tp'), P('dp')),
        check_vma=False,
    )
```

```python
import functools
import math

import jax
import jax.numpy as jnp
from jax import lax
from jax.experimental import pallas as pl
from jax.experimental.layout import Layout, with_layout_constraint
from jax.experimental.pallas import tpu as pltpu
from jax.sharding import PartitionSpec as P


EPS = 1e-6
f32 = jnp.float32
bf16 = jnp.bfloat16
LANES = 128
SPLIT = (10, 6)


def _gather_kernel(S, own_r, left_r, right_r, own_c, left_c, right_c, wt_ref, ss_ref, du_r, du_c, w_r, w_c, sum_ref, vdu, vw, rbuf, mid, cbuf,
                   lsem, ssem, rsem, wssem, wrsem, tssem, trsem):
    me = lax.axis_index('tp')
    c = lax.rem(me, 2)
    x = lax.rem(me // 2, S)
    y = me // (2 * S)
    F = own_r.shape[0]
    dev = lambda yy, xx, cc: (yy * S + xx) * 2 + cc
    rot = lambda v, k: lax.rem(v + k, S)

    barrier = pltpu.get_barrier_semaphore()
    others = [dev(y, x, 1 - c)]
    for k in range(1, S):
        for cc in range(2):
            others += [dev(y, rot(x, k), cc), dev(rot(y, k), x, cc)]
    for p in others:
        pl.semaphore_signal(barrier, inc=1, device_id={'tp': p})
    pl.semaphore_wait(barrier, len(others))

    i_row = lax.rem(me, 2 * S)
    row = []
    for k in range(1, 2 * S):
        cp = pltpu.make_async_remote_copy(
            ss_ref, rbuf.at[i_row], tssem.at[k], trsem.at[k], device_id={'tp': y * 2 * S + lax.rem(i_row + k, 2 * S)}
        )
        cp.start()
        row.append(cp)
    rbuf[i_row] = ss_ref[...]

    Bw = w_r.shape[3]
    wblock = lambda b: wt_ref.at[:, pl.ds(pl.multiple_of(b * Bw, Bw), Bw)]
    outs = []
    schemes = []
    for j, (pos, buf, wbuf, src) in enumerate(
        ((x, du_r, w_r, (own_r, left_r, right_r)), (y, du_c, w_c, (own_c, left_c, right_c)))
    ):
        at = (lambda k, cc: dev(y, rot(x, k), cc)) if j == 0 else (lambda k, cc: dev(rot(y, k), x, cc))
        slots = [2 * rot(pos, k) + c for k in (0, S - 1, 1, 2)]
        schemes.append((j, pos, buf, wbuf, at, src, slots))

    def send(j, i, src, dst, p):
        cp = pltpu.make_async_remote_copy(src, dst, ssem.at[j, i], rsem.at[j, i], device_id={'tp': p})
        cp.start()
        outs.append(cp)
        return cp

    halves = []
    for j, pos, buf, wbuf, at, src, slots in schemes:
        top, low = pl.ds(0, F // 2), pl.ds(F // 2, F // 2)
        a = send(j, 0, src[1].at[top], buf.at[slots[1], top], at(1, c))
        b = send(j, 1, src[2].at[low], buf.at[slots[2], low], at(S - 1, c))
        halves.append((a, b))
    local = []
    for j, pos, buf, wbuf, at, src, slots in schemes:
        moves = [(src[i], vdu.at[j, i], buf.at[slots[i]]) for i in range(3)]
        for t in range(S):
            own = wblock(dev(t, x, c) if j == 0 else dev(y, t, c))
            moves.append((own, vw.at[j, t], wbuf.at[lax.rem(t + S - (y if j == 0 else x), S), slots[0]]))
        for i, (a, v, dst) in enumerate(moves):
            cp = pltpu.make_async_copy(a, v, lsem.at[j, i])
            cp.start()
            local.append((cp, v, dst, j, i))
    for k in [1, S - 1, 0] + list(range(2, S - 1)):
        for j, pos, buf, wbuf, at, src, slots in schemes:
            for cc in range(2):
                oc = c if cc == 0 else 1 - c
                if k == 0 and cc == 0:
                    continue
                for t in range(S):
                    blk = wblock(dev(t, rot(x, k), oc) if j == 0 else dev(rot(y, k), t, oc))
                    cp = pltpu.make_async_remote_copy(
                        blk, wbuf.at[lax.rem(t + S - (y if j == 0 else x), S), slots[0]], wssem.at[j, 2 * k + cc, t], wrsem.at[j, 2 * k + cc, t], device_id={'tp': at(k, oc)}
                    )
                    cp.start()
                    outs.append(cp)
        if k == 1:
            for j, pos, buf, wbuf, at, src, slots in schemes:
                for i in range(3):
                    send(j, 2 + i, src[i], buf.at[slots[i]], at(0, 1 - c))
        if k == S - 1:
            for cp in row:
                cp.wait()
            total = rbuf[0]
            for t in range(1, 2 * S):
                total = total + rbuf[t]
            mid[...] = total
            cbuf[y] = total
            col = []
            for t in range(1, S):
                cp = pltpu.make_async_remote_copy(
                    mid, cbuf.at[y], tssem.at[2 * S + t], trsem.at[2 * S + t], device_id={'tp': dev(rot(y, t), x, c)}
                )
                cp.start()
                col.append(cp)
    for cp, v, dst, j, i in local:
        cp.wait()
    back = []
    for cp, v, dst, j, i in local:
        cb = pltpu.make_async_copy(v, dst, lsem.at[j, i + 8])
        cb.start()
        back.append(cb)
    for j, pos, buf, wbuf, at, src, slots in schemes:
        a, b = halves[j]
        a.wait_recv()
        b.wait_recv()
        send(j, 5, buf.at[slots[3]], buf.at[slots[3]], at(0, 1 - c))
    early = {id(cp) for pair in halves for cp in pair}
    for cp in outs:
        cp.wait_send()
        if id(cp) not in early:
            cp.wait_recv()
    for cb in back:
        cb.wait()
    for cp in col:
        cp.wait()
    total = cbuf[0]
    for t in range(1, S):
        total = total + cbuf[t]
    sum_ref[...] = total


def _gather(du_r, du_c, wt, ss, S, cid):
    F, H = du_r[0].shape
    G = 2 * S * S
    B = wt.shape[1] // G
    R = ss.shape[0]
    anyspace = pl.BlockSpec(memory_space=pl.ANY)
    vm = pl.BlockSpec(memory_space=pltpu.VMEM)
    dma = pltpu.SemaphoreType.DMA
    return pl.pallas_call(
        functools.partial(_gather_kernel, S),
        out_shape=(
            jax.ShapeDtypeStruct((2 * S, F, H), bf16),
            jax.ShapeDtypeStruct((2 * S, F, H), bf16),
            jax.ShapeDtypeStruct((S, 2 * S, F, B), bf16),
            jax.ShapeDtypeStruct((S, 2 * S, F, B), bf16),
            jax.ShapeDtypeStruct((R, LANES), f32),
        ),
        in_specs=[anyspace] * 7 + [vm],
        out_specs=(anyspace,) * 4 + (vm,),
        scratch_shapes=[
            pltpu.VMEM((2, 3, F, H), bf16),
            pltpu.VMEM((2, S, F, B), bf16),
            pltpu.VMEM((2 * S, R, LANES), f32),
            pltpu.VMEM((R, LANES), f32),
            pltpu.VMEM((S, R, LANES), f32),
            dma((2, 16)), dma((2, 8)), dma((2, 8)), dma((2, 2 * S, S)), dma((2, 2 * S, S)), dma((3 * S,)), dma((3 * S,)),
        ],
        compiler_params=pltpu.CompilerParams(collective_id=cid, has_side_effects=True),
        name='gather_du_w',
    )(*du_r, *du_c, wt, ss)


def _stats_kernel(C, ROW, S, Q, x_ref, sum_ref, gat_ref, rbuf, mid, cbuf, ssem, rsem, ssem2, rsem2):
    me = lax.axis_index('tp')
    y, i = me // ROW, lax.rem(me, ROW)
    barrier = pltpu.get_barrier_semaphore()
    row_peers = [y * ROW + lax.rem(i + k, ROW) for k in range(1, ROW)]
    col_peers = [lax.rem(y + k, C) * ROW + i for k in range(1, C)]
    for p in row_peers + col_peers:
        pl.semaphore_signal(barrier, inc=1, device_id={'tp': p})
    pl.semaphore_wait(barrier, ROW + C - 2)

    copies = []
    for k, p in enumerate(row_peers):
        cp = pltpu.make_async_remote_copy(x_ref, rbuf.at[i], ssem.at[k], rsem.at[k], device_id={'tp': p})
        cp.start()
        copies.append(cp)
    rbuf[i] = x_ref[...]
    for cp in copies:
        cp.wait()
    total = rbuf[0, :S]
    for s in range(1, ROW):
        total = total + rbuf[s, :S]
    mid[:S] = total
    if Q:
        for s in range(ROW):
            mid[S + s * Q:S + (s + 1) * Q] = rbuf[s, S:]

    copies = []
    for k, p in enumerate(col_peers):
        cp = pltpu.make_async_remote_copy(mid, cbuf.at[y], ssem2.at[k], rsem2.at[k], device_id={'tp': p})
        cp.start()
        copies.append(cp)
    cbuf[y] = mid[...]
    for cp in copies:
        cp.wait()
    total = cbuf[0, :S]
    for s in range(1, C):
        total = total + cbuf[s, :S]
    sum_ref[...] = total
    if Q:
        for s in range(C):
            gat_ref[s * ROW * Q:(s + 1) * ROW * Q] = cbuf[s, S:]
    else:
        gat_ref[...] = jnp.zeros_like(gat_ref)


def _stats(x, C, Q, cid):
    ROW = 2 * C
    R = x.shape[0]
    S = R - Q
    M = S + ROW * Q
    q_out = C * ROW * Q if Q else 8
    vm = pl.BlockSpec(memory_space=pltpu.VMEM)
    return pl.pallas_call(
        functools.partial(_stats_kernel, C, ROW, S, Q),
        out_shape=(jax.ShapeDtypeStruct((S, LANES), f32), jax.ShapeDtypeStruct((q_out, LANES), f32)),
        in_specs=[vm],
        out_specs=(vm, vm),
        scratch_shapes=[
            pltpu.VMEM((ROW, R, LANES), f32),
            pltpu.VMEM((M, LANES), f32),
            pltpu.VMEM((C, M, LANES), f32),
            pltpu.SemaphoreType.DMA((ROW - 1,)),
            pltpu.SemaphoreType.DMA((ROW - 1,)),
            pltpu.SemaphoreType.DMA((C - 1,)),
            pltpu.SemaphoreType.DMA((C - 1,)),
        ],
        compiler_params=pltpu.CompilerParams(collective_id=cid, has_side_effects=True),
    )(x)


def rowmajor(v):
    return with_layout_constraint(v, Layout(major_to_minor=tuple(range(v.ndim))))


def solution(mesh):
    G = mesh.shape['tp']
    S = math.isqrt(G // 2)
    C, ROW = S, 2 * S

    def shift(j, k):
        out = []
        for i in range(G):
            y, x, c = i // ROW, i // 2 % S, i % 2
            t = ((y + k) % S, x, c) if j == 0 else (y, (x + k) % S, c)
            out.append((i, (t[0] * S + t[1]) * 2 + t[2]))
        return out

    def body(ids, E, g, W, du, dres):
        K, T = ids.shape
        D = g.shape[0]
        B = E.shape[1]
        F = W.shape[1]
        N = K * T
        TL = T // G
        r = lax.axis_index('tp')
        idf = ids.reshape(N)
        gl = lax.dynamic_slice_in_dim(g, r * B, B).astype(f32)
        gf = g.astype(f32)
        duf = du.reshape(N, F)
        k0, k1 = SPLIT
        du_rc = []
        for j in range(2):
            own = rowmajor(duf[j * (N // 2):(j + 1) * (N // 2)].T)
            du_rc.append((own, lax.ppermute(own, 'tp', shift(1 - j, 1)), lax.ppermute(own, 'tp', shift(1 - j, S - 1))))
        xl0 = rowmajor(jnp.take(E, idf[:k0 * T], axis=0))
        x0 = lax.all_gather(xl0, 'tp', axis=1, tiled=True)
        xl1 = rowmajor(jnp.take(E, idf[k0 * T:], axis=0))
        x1 = lax.all_gather(xl1, 'tp', axis=1, tiled=True)
        sq = lambda v: jnp.sum(v.astype(f32) * v.astype(f32), axis=-1).reshape(-1, LANES)
        ss = jnp.concatenate([sq(xl0), sq(xl1)], axis=0)
        xl = jnp.concatenate([xl0, xl1], axis=0)
        duR, duC, wR, wC, ss = _gather(*du_rc, W.T, ss, S, 2)
        rs = lax.rsqrt(ss.reshape(N) / D + EPS)[:, None]
        duR, duC, wR, wC, rs, dres = lax.optimization_barrier((duR, duC, wR, wC, rs, dres))
        dt = dres.reshape(K * TL, G, B).transpose(1, 0, 2)
        dt = lax.all_to_all(dt, 'tp', 0, 0, tiled=True)
        parts = []
        for j, (a, w) in enumerate(((duR, wR), (duC, wC))):
            p = jnp.einsum('kt,ykb->ytb', a.reshape(ROW * F, N // 2), w.reshape(S, ROW * F, B),
                           preferred_element_type=f32).astype(bf16)
            p = rowmajor(p)
            ps = []
            for k in range(1, S + 1):
                k = k % S
                ps.append(lax.ppermute(p[k], 'tp', shift(j, k)) if k else p[k])
            parts.append(ps)
        us, xss = [], []

        def forward(xg, at, kc, dW):
            sl = slice(at * T, (at + kc) * T)
            xss.append(lax.dynamic_slice_in_dim(xg.reshape(kc, T, D), r * TL, TL, axis=1))
            n = (xg.astype(f32) * rs[sl] * gf).astype(bf16)
            us.append(jnp.dot(n, W, preferred_element_type=f32).astype(bf16))
            w = jnp.einsum('td,tf->df', n, duf[sl], preferred_element_type=f32)
            return w if dW is None else dW + w

        dW = forward(x0, 0, k0, None)
        dW, us[0], parts, dt = lax.optimization_barrier((dW, us[0], parts, dt))
        dl = rowmajor(rowmajor(dt.reshape(G, K, TL, B).transpose(1, 0, 2, 3)).reshape(N, B))
        dn = jnp.concatenate([sum(p.astype(f32) for p in ps) for ps in parts], axis=0)
        nh = xl.astype(f32) * rs
        gdn = gl * dn
        pk = jnp.concatenate([jnp.sum(nh * gdn, axis=-1).reshape(N // LANES, LANES),
                              jnp.sum(dn * nh, axis=0).reshape(B // LANES, LANES)], axis=0)
        ms, dgs = _stats(pk, C, B // LANES, 1)
        dg = dgs.reshape(D)
        dx = dl.astype(f32) + rs * (gdn - nh * (ms.reshape(N) / D)[:, None])
        dE = jnp.zeros(E.shape, f32).at[idf].add(dx)
        x1, dW, dE = lax.optimization_barrier((x1, dW, dE))
        dW = forward(x1, k0, k1, dW)
        u = jnp.concatenate(us, axis=0).reshape(K, T, F)
        xs = jnp.concatenate(xss, axis=0)
        return u, xs, dE, dW, dg

    return jax.shard_map(
        body,
        mesh=mesh,
        in_specs=(P('dp', None), P(None, 'tp'), P(), P(None, 'tp'), P('dp', None, 'tp'), P('dp', 'tp', None)),
        out_specs=(P('dp', None, 'tp'), P('dp', 'tp', None), P('dp', 'tp'), P('dp', 'tp'), P('dp')),
        check_vma=False,
    )
```

```python
import functools
import math

import jax
import jax.numpy as jnp
from jax import lax
from jax.experimental import pallas as pl
from jax.experimental.layout import Layout, with_layout_constraint
from jax.experimental.pallas import tpu as pltpu
from jax.sharding import PartitionSpec as P


EPS = 1e-6
f32 = jnp.float32
bf16 = jnp.bfloat16
LANES = 128
SPLIT = (10, 6)


def _gather_kernel(S, own_r, left_r, right_r, own_c, left_c, right_c, wt_ref, ss_ref, du_r, du_c, w_r, w_c, sum_ref, vdu, vw, rbuf, mid, cbuf,
                   lsem, ssem, rsem, wssem, wrsem, tssem, trsem):
    me = lax.axis_index('tp')
    c = lax.rem(me, 2)
    x = lax.rem(me // 2, S)
    y = me // (2 * S)
    F = own_r.shape[0]
    dev = lambda yy, xx, cc: (yy * S + xx) * 2 + cc
    rot = lambda v, k: lax.rem(v + k, S)

    barrier = pltpu.get_barrier_semaphore()
    others = [dev(y, x, 1 - c)]
    for k in range(1, S):
        for cc in range(2):
            others += [dev(y, rot(x, k), cc), dev(rot(y, k), x, cc)]
    for p in others:
        pl.semaphore_signal(barrier, inc=1, device_id={'tp': p})
    pl.semaphore_wait(barrier, len(others))

    i_row = lax.rem(me, 2 * S)
    row = []
    for k in range(1, 2 * S):
        cp = pltpu.make_async_remote_copy(
            ss_ref, rbuf.at[i_row], tssem.at[k], trsem.at[k], device_id={'tp': y * 2 * S + lax.rem(i_row + k, 2 * S)}
        )
        cp.start()
        row.append(cp)
    rbuf[i_row] = ss_ref[...]

    Bw = w_r.shape[3]
    wblock = lambda b: wt_ref.at[:, pl.ds(pl.multiple_of(b * Bw, Bw), Bw)]
    outs = []
    schemes = []
    for j, (pos, buf, wbuf, src) in enumerate(
        ((x, du_r, w_r, (own_r, left_r, right_r)), (y, du_c, w_c, (own_c, left_c, right_c)))
    ):
        at = (lambda k, cc: dev(y, rot(x, k), cc)) if j == 0 else (lambda k, cc: dev(rot(y, k), x, cc))
        slots = [2 * rot(pos, k) + c for k in (0, S - 1, 1, 2)]
        schemes.append((j, pos, buf, wbuf, at, src, slots))

    def send(j, i, src, dst, p):
        cp = pltpu.make_async_remote_copy(src, dst, ssem.at[j, i], rsem.at[j, i], device_id={'tp': p})
        cp.start()
        outs.append(cp)
        return cp

    halves = []
    for j, pos, buf, wbuf, at, src, slots in schemes:
        top, low = pl.ds(0, F // 2), pl.ds(F // 2, F // 2)
        a = send(j, 0, src[1].at[top], buf.at[slots[1], top], at(1, c))
        b = send(j, 1, src[2].at[low], buf.at[slots[2], low], at(S - 1, c))
        halves.append((a, b))
    local = []
    for j, pos, buf, wbuf, at, src, slots in schemes:
        moves = [(src[i], vdu.at[j, i], buf.at[slots[i]]) for i in range(3)]
        for t in range(S):
            own = wblock(dev(t, x, c) if j == 0 else dev(y, t, c))
            moves.append((own, vw.at[j, t], wbuf.at[lax.rem(t + S - (y if j == 0 else x), S), slots[0]]))
        for i, (a, v, dst) in enumerate(moves):
            cp = pltpu.make_async_copy(a, v, lsem.at[j, i])
            cp.start()
            local.append((cp, v, dst, j, i))
    for k in [1, S - 1, 0] + list(range(2, S - 1)):
        for j, pos, buf, wbuf, at, src, slots in schemes:
            for cc in range(2):
                oc = c if cc == 0 else 1 - c
                if k == 0 and cc == 0:
                    continue
                for t in range(S):
                    blk = wblock(dev(t, rot(x, k), oc) if j == 0 else dev(rot(y, k), t, oc))
                    cp = pltpu.make_async_remote_copy(
                        blk, wbuf.at[lax.rem(t + S - (y if j == 0 else x), S), slots[0]], wssem.at[j, 2 * k + cc, t], wrsem.at[j, 2 * k + cc, t], device_id={'tp': at(k, oc)}
                    )
                    cp.start()
                    outs.append(cp)
        if k == 1:
            for j, pos, buf, wbuf, at, src, slots in schemes:
                for i in range(3):
                    send(j, 2 + i, src[i], buf.at[slots[i]], at(0, 1 - c))
        if k == S - 1:
            for cp in row:
                cp.wait()
            total = rbuf[0]
            for t in range(1, 2 * S):
                total = total + rbuf[t]
            mid[...] = total
            cbuf[y] = total
            col = []
            for t in range(1, S):
                cp = pltpu.make_async_remote_copy(
                    mid, cbuf.at[y], tssem.at[2 * S + t], trsem.at[2 * S + t], device_id={'tp': dev(rot(y, t), x, c)}
                )
                cp.start()
                col.append(cp)
    for cp, v, dst, j, i in local:
        cp.wait()
    back = []
    for cp, v, dst, j, i in local:
        cb = pltpu.make_async_copy(v, dst, lsem.at[j, i + 8])
        cb.start()
        back.append(cb)
    for j, pos, buf, wbuf, at, src, slots in schemes:
        a, b = halves[j]
        a.wait_recv()
        b.wait_recv()
        send(j, 5, buf.at[slots[3]], buf.at[slots[3]], at(0, 1 - c))
    early = {id(cp) for pair in halves for cp in pair}
    for cp in outs:
        cp.wait_send()
        if id(cp) not in early:
            cp.wait_recv()
    for cb in back:
        cb.wait()
    for cp in col:
        cp.wait()
    total = cbuf[0]
    for t in range(1, S):
        total = total + cbuf[t]
    sum_ref[...] = total


def _gather(du_r, du_c, wt, ss, S, cid):
    F, H = du_r[0].shape
    G = 2 * S * S
    B = wt.shape[1] // G
    R = ss.shape[0]
    anyspace = pl.BlockSpec(memory_space=pl.ANY)
    vm = pl.BlockSpec(memory_space=pltpu.VMEM)
    dma = pltpu.SemaphoreType.DMA
    return pl.pallas_call(
        functools.partial(_gather_kernel, S),
        out_shape=(
            jax.ShapeDtypeStruct((2 * S, F, H), bf16),
            jax.ShapeDtypeStruct((2 * S, F, H), bf16),
            jax.ShapeDtypeStruct((S, 2 * S, F, B), bf16),
            jax.ShapeDtypeStruct((S, 2 * S, F, B), bf16),
            jax.ShapeDtypeStruct((R, LANES), f32),
        ),
        in_specs=[anyspace] * 7 + [vm],
        out_specs=(anyspace,) * 4 + (vm,),
        scratch_shapes=[
            pltpu.VMEM((2, 3, F, H), bf16),
            pltpu.VMEM((2, S, F, B), bf16),
            pltpu.VMEM((2 * S, R, LANES), f32),
            pltpu.VMEM((R, LANES), f32),
            pltpu.VMEM((S, R, LANES), f32),
            dma((2, 16)), dma((2, 8)), dma((2, 8)), dma((2, 2 * S, S)), dma((2, 2 * S, S)), dma((3 * S,)), dma((3 * S,)),
        ],
        compiler_params=pltpu.CompilerParams(collective_id=cid, has_side_effects=True),
        name='gather_du_w',
    )(*du_r, *du_c, wt, ss)


def _stats_kernel(C, ROW, S, Q, x_ref, sum_ref, gat_ref, rbuf, mid, cbuf, ssem, rsem, ssem2, rsem2):
    me = lax.axis_index('tp')
    y, i = me // ROW, lax.rem(me, ROW)
    barrier = pltpu.get_barrier_semaphore()
    row_peers = [y * ROW + lax.rem(i + k, ROW) for k in range(1, ROW)]
    col_peers = [lax.rem(y + k, C) * ROW + i for k in range(1, C)]
    for p in row_peers + col_peers:
        pl.semaphore_signal(barrier, inc=1, device_id={'tp': p})
    pl.semaphore_wait(barrier, ROW + C - 2)

    copies = []
    for k, p in enumerate(row_peers):
        cp = pltpu.make_async_remote_copy(x_ref, rbuf.at[i], ssem.at[k], rsem.at[k], device_id={'tp': p})
        cp.start()
        copies.append(cp)
    rbuf[i] = x_ref[...]
    for cp in copies:
        cp.wait()
    total = rbuf[0, :S]
    for s in range(1, ROW):
        total = total + rbuf[s, :S]
    mid[:S] = total
    if Q:
        for s in range(ROW):
            mid[S + s * Q:S + (s + 1) * Q] = rbuf[s, S:]

    copies = []
    for k, p in enumerate(col_peers):
        cp = pltpu.make_async_remote_copy(mid, cbuf.at[y], ssem2.at[k], rsem2.at[k], device_id={'tp': p})
        cp.start()
        copies.append(cp)
    cbuf[y] = mid[...]
    for cp in copies:
        cp.wait()
    total = cbuf[0, :S]
    for s in range(1, C):
        total = total + cbuf[s, :S]
    sum_ref[...] = total
    if Q:
        for s in range(C):
            gat_ref[s * ROW * Q:(s + 1) * ROW * Q] = cbuf[s, S:]
    else:
        gat_ref[...] = jnp.zeros_like(gat_ref)


def _stats(x, C, Q, cid):
    ROW = 2 * C
    R = x.shape[0]
    S = R - Q
    M = S + ROW * Q
    q_out = C * ROW * Q if Q else 8
    vm = pl.BlockSpec(memory_space=pltpu.VMEM)
    return pl.pallas_call(
        functools.partial(_stats_kernel, C, ROW, S, Q),
        out_shape=(jax.ShapeDtypeStruct((S, LANES), f32), jax.ShapeDtypeStruct((q_out, LANES), f32)),
        in_specs=[vm],
        out_specs=(vm, vm),
        scratch_shapes=[
            pltpu.VMEM((ROW, R, LANES), f32),
            pltpu.VMEM((M, LANES), f32),
            pltpu.VMEM((C, M, LANES), f32),
            pltpu.SemaphoreType.DMA((ROW - 1,)),
            pltpu.SemaphoreType.DMA((ROW - 1,)),
            pltpu.SemaphoreType.DMA((C - 1,)),
            pltpu.SemaphoreType.DMA((C - 1,)),
        ],
        compiler_params=pltpu.CompilerParams(collective_id=cid, has_side_effects=True),
    )(x)


def rowmajor(v):
    return with_layout_constraint(v, Layout(major_to_minor=tuple(range(v.ndim))))


def solution(mesh):
    G = mesh.shape['tp']
    S = math.isqrt(G // 2)
    C, ROW = S, 2 * S

    def shift(j, k):
        out = []
        for i in range(G):
            y, x, c = i // ROW, i // 2 % S, i % 2
            t = ((y + k) % S, x, c) if j == 0 else (y, (x + k) % S, c)
            out.append((i, (t[0] * S + t[1]) * 2 + t[2]))
        return out

    def body(ids, E, g, W, du, dres):
        K, T = ids.shape
        D = g.shape[0]
        B = E.shape[1]
        F = W.shape[1]
        N = K * T
        TL = T // G
        r = lax.axis_index('tp')
        idf = ids.reshape(N)
        gl = lax.dynamic_slice_in_dim(g, r * B, B).astype(f32)
        gf = g.astype(f32)
        duf = du.reshape(N, F)
        k0, k1 = SPLIT
        du_rc = []
        for j in range(2):
            own = rowmajor(duf[j * (N // 2):(j + 1) * (N // 2)].T)
            du_rc.append((own, lax.ppermute(own, 'tp', shift(1 - j, 1)), lax.ppermute(own, 'tp', shift(1 - j, S - 1))))
        xl0 = rowmajor(jnp.take(E, idf[:k0 * T], axis=0))
        x0 = lax.all_gather(xl0, 'tp', axis=1, tiled=True)
        xl1 = rowmajor(jnp.take(E, idf[k0 * T:], axis=0))
        x1 = lax.all_gather(xl1, 'tp', axis=1, tiled=True)
        sq = lambda v: jnp.sum(v.astype(f32) * v.astype(f32), axis=-1).reshape(-1, LANES)
        ss = jnp.concatenate([sq(xl0), sq(xl1)], axis=0)
        xl = jnp.concatenate([xl0, xl1], axis=0)
        duR, duC, wR, wC, ss = _gather(*du_rc, W.T, ss, S, 2)
        rs = lax.rsqrt(ss.reshape(N) / D + EPS)[:, None]
        duR, duC, wR, wC, rs, dres = lax.optimization_barrier((duR, duC, wR, wC, rs, dres))
        dt = dres.reshape(K * TL, G, B).transpose(1, 0, 2)
        dt = lax.all_to_all(dt, 'tp', 0, 0, tiled=True)
        parts = []
        for j, (a, w) in enumerate(((duR, wR), (duC, wC))):
            p = jnp.einsum('kt,ykb->ytb', a.reshape(ROW * F, N // 2), w.reshape(S, ROW * F, B),
                           preferred_element_type=f32).astype(bf16)
            p = rowmajor(p)
            ps = []
            for k in range(1, S + 1):
                k = k % S
                ps.append(lax.ppermute(p[k], 'tp', shift(j, k)) if k else p[k])
            parts.append(ps)
        us, xss = [], []

        def forward(xg, at, kc, dW):
            sl = slice(at * T, (at + kc) * T)
            xss.append(lax.dynamic_slice_in_dim(xg.reshape(kc, T, D), r * TL, TL, axis=1))
            n = (xg.astype(f32) * rs[sl] * gf).astype(bf16)
            us.append(jnp.dot(n, W, preferred_element_type=f32).astype(bf16))
            w = jnp.einsum('td,tf->df', n, duf[sl], preferred_element_type=f32)
            return w if dW is None else dW + w

        dW = forward(x0, 0, k0, None)
        dW, us[0], parts, dt = lax.optimization_barrier((dW, us[0], parts, dt))
        dl = rowmajor(rowmajor(dt.reshape(G, K, TL, B).transpose(1, 0, 2, 3)).reshape(N, B))
        dn = jnp.concatenate([sum(p.astype(f32) for p in ps) for ps in parts], axis=0)
        nh = xl.astype(f32) * rs
        gdn = gl * dn
        pk = jnp.concatenate([jnp.sum(nh * gdn, axis=-1).reshape(N // LANES, LANES),
                              jnp.sum(dn * nh, axis=0).reshape(B // LANES, LANES)], axis=0)
        ms, dgs = _stats(pk, C, B // LANES, 1)
        dg = dgs.reshape(D)
        dx = dl.astype(f32) + rs * (gdn - nh * (ms.reshape(N) / D)[:, None])
        dE = jnp.zeros(E.shape, f32).at[idf].add(dx)
        late = ((0, k1, 0), (0, 0, 0), (0, 0, 0))
        u = lax.pad(us[0].reshape(k0, T, F), jnp.zeros((), bf16), late)
        xs = lax.pad(xss[0], jnp.zeros((), bf16), late)
        x1, dW, dE, u, xs = lax.optimization_barrier((x1, dW, dE, u, xs))
        dW = forward(x1, k0, k1, dW)
        u = lax.dynamic_update_slice(u, us[1].reshape(k1, T, F), (k0, 0, 0))
        xs = lax.dynamic_update_slice(xs, xss[1], (k0, 0, 0))
        return u, xs, dE, dW, dg

    return jax.shard_map(
        body,
        mesh=mesh,
        in_specs=(P('dp', None), P(None, 'tp'), P(), P(None, 'tp'), P('dp', None, 'tp'), P('dp', 'tp', None)),
        out_specs=(P('dp', None, 'tp'), P('dp', 'tp', None), P('dp', 'tp'), P('dp', 'tp'), P('dp')),
        check_vma=False,
    )
```
